32 devices in a mesh: grp: 2 (over core), tp: 4 (over y, x), src: 4 (over z).
Axes of the slice: x: 2, y: 2, z: 4, core: 2. Of those that a mesh axis runs over, the one named last changes fastest.
Arguments:
- hidden_in: bfloat16 [512, 5120], P(('grp', 'src')), may hold values from -6 to 6
- attn_gain: float32 [5120], replicated, may hold values from 0.5 to 1.5
- w_qkv: int32 [1280, 5120], P(None, 'tp'), may hold values from -2147483648 to 2147483646
- qkv_scale: float32 [5120], P('tp'), may hold values from 0.0001118034 to 0.00041926274
- q_gain: float32 [128], replicated, may hold values from 0.25 to 1.75
- k_gain: float32 [128], replicated, may hold values from 0.1 to 1.9
- key_cache: bfloat16 [8, 64, 128, 512], P(('grp', 'src'), 'tp'), may hold values from -400 to 400
- value_cache: bfloat16 [8, 64, 128, 512], P(('grp', 'src'), 'tp'), may hold values from -9 to 9
- lengths: int32 [8, 64], P(('grp', 'src'), 'tp'), may hold values from 1 to 128, as said below
- w_out: int32 [1024, 5120], P('tp'), may hold values from -2147483648 to 2147483646
- out_scale: float32 [5120], replicated, may hold values from 0.0003125 to 0.00125
- mlp_gain: float32 [5120], replicated, may hold values from 0.5 to 1.5
- w_gate: int32 [1280, 12800], P(('grp', 'src'), 'tp'), may hold values from -2147483648 to 2147483646
- w_up: int32 [1280, 12800], P(('grp', 'src'), 'tp'), may hold values from -2147483648 to 2147483646
- gate_scale: float32 [12800], P('tp'), may hold values from 0.0001118034 to 0.00041926274
- up_scale: float32 [12800], P('tp'), may hold values from 0.0001118034 to 0.00041926274
- w_down: int32 [3200, 5120], P('tp', ('grp', 'src')), may hold values from -2147483648 to 2147483646
- down_scale: float32 [5120], replicated, may hold values from 0.00013258251 to 0.00053033006
Outputs:
- layer_out: bfloat16 [512, 5120], P(('grp', 'src'), 'tp')
The draws below stay inside these ranges and needn't reach their ends.
Inputs may be any that keep to these rules, and one draw needn't show every extreme that they name: `lengths`: some sequence has exactly 128 cached positions.
All inputs are finite; a program needn't handle non-finite values.
Results may differ from the reference program's by a relative error of at most 0.028.
Values may be sent and summed in bfloat16 or wider, within the bound.
A program may use at most 128 MiB of HBM per device.

```python
import math
import jax
import jax.numpy as jnp
from jax import lax

D = 5120
QUERY_HEADS = 32
KEY_VALUE_HEADS = 4
HEAD_SIZE = 128
FFW = 12800
B_DEV = 64
CACHE_POSITIONS = 128
NGROUPS = 8
B = 512
QUERY_COLUMNS = 4096
KEY_COLUMNS = 512
QKV = 5120


def draw_key_cache(key, part):
    first_key = jax.random.fold_in(jax.random.fold_in(key, 11), 0)
    normal_part = jax.random.normal(first_key, (NGROUPS, B_DEV, CACHE_POSITIONS, KEY_COLUMNS), jnp.float32)
    return jnp.clip(normal_part, -6.0, 6.0).astype(jnp.bfloat16)


def draw_lengths(key, part):
    first_key, second_key = jax.random.split(jax.random.fold_in(key, 23))
    base_lengths = jax.random.randint(first_key, (NGROUPS * B_DEV,), 1, CACHE_POSITIONS + 1)
    longest_slot = jax.random.randint(second_key, (), 0, NGROUPS * B_DEV)
    flat_lengths = jnp.where(jnp.arange(NGROUPS * B_DEV) == longest_slot, CACHE_POSITIONS, base_lengths)
    return flat_lengths.reshape(NGROUPS, B_DEV).astype(jnp.int32)


def set_ends(array, stream_key, least, largest):
    longest = array.shape.index(max(array.shape))
    spots = []
    for shift in (0, 1):
        where = [jax.random.randint(jax.random.fold_in(stream_key, axis), (), 0, length) for axis, length in enumerate(array.shape)]
        where[longest] = (where[longest] + shift) % array.shape[longest]
        spots.append(tuple(where))
    return array.at[spots[0]].set(least).at[spots[1]].set(largest)


def steps_of(own_key, extent, pieces, least, top_value):
    level, own = 1.0, jax.random.fold_in(own_key, 6)
    for axis_at, blocks in pieces:
        draws = jnp.exp(jax.random.uniform(jax.random.fold_in(own, axis_at), (blocks,), jnp.float32, least / len(pieces), top_value / len(pieces)))
        level = level * jnp.repeat(draws, extent[axis_at] // blocks).reshape([-1 if axis == axis_at else 1 for axis in range(len(extent))])
    return level


def scatter_about(rng, dims, width, bound, cuts=(), kind=jnp.bfloat16):
    loudness = steps_of(rng, dims, cuts, -0.22, 0.18) if cuts else 1.0
    result = jax.random.normal(rng, dims, jnp.float32) * width * loudness
    return jnp.minimum(jnp.maximum(result, -bound), bound).astype(kind)


def setup_inputs(seed: int = 0) -> dict:
    arg_keys = jax.random.split(jax.random.key(seed), 19)
    hidden_in = scatter_about(arg_keys[0], (B, D), 1.0, 6.0, ((0, 8),))
    attn_gain = jnp.clip(1.0 + 0.1 * jax.random.normal(arg_keys[1], (D,), jnp.float32), 0.5, 1.5)
    w_qkv = set_ends(jax.random.randint(arg_keys[2], (D // 4, QKV), -2147483648, 2147483647), jax.random.fold_in(arg_keys[2], 1), -2147483648, 2147483646).astype(jnp.int32)
    qkv_scale = jnp.clip(jnp.exp(math.log(0.00041926274) - 1.32175583 * jax.random.uniform(arg_keys[3], (QKV,), jnp.float32) ** steps_of(arg_keys[3], (QKV,), ((0, 4),), -0.2, 0.2)), 0.0001118034, 0.00041926274)
    q_gain = jnp.clip(1.0 + 0.15 * jax.random.normal(arg_keys[4], (HEAD_SIZE,), jnp.float32), 0.25, 1.75)
    k_gain = jnp.clip(1.0 + 0.18 * jax.random.normal(arg_keys[5], (HEAD_SIZE,), jnp.float32), 0.1, 1.9)
    key_cache = draw_key_cache(jax.random.fold_in(arg_keys[18], 71), 0)
    value_cache = scatter_about(arg_keys[7], (NGROUPS, B_DEV, CACHE_POSITIONS, KEY_COLUMNS), 1.5, 9.0, ((0, 8), (1, 4)))
    lengths = draw_lengths(jax.random.fold_in(arg_keys[18], 71), 0)
    w_out = set_ends(jax.random.randint(arg_keys[9], (QUERY_COLUMNS // 4, D), -2147483648, 2147483647), jax.random.fold_in(arg_keys[9], 1), -2147483648, 2147483646).astype(jnp.int32)
    out_scale = jnp.clip(jnp.exp(jax.random.uniform(arg_keys[10], (D,), jnp.float32, math.log(0.0003125), math.log(0.00125))), 0.0003125, 0.00125)
    mlp_gain = jnp.clip(1.0 + 0.1 * jax.random.normal(arg_keys[11], (D,), jnp.float32), 0.5, 1.5)
    w_gate = set_ends(jax.random.randint(arg_keys[12], (D // 4, FFW), -2147483648, 2147483647), jax.random.fold_in(arg_keys[12], 1), -2147483648, 2147483646).astype(jnp.int32)
    w_up = set_ends(jax.random.randint(arg_keys[13], (D // 4, FFW), -2147483648, 2147483647), jax.random.fold_in(arg_keys[13], 1), -2147483648, 2147483646).astype(jnp.int32)
    gate_scale = jnp.clip(jnp.exp(math.log(0.00041926274) - 1.32175583 * jax.random.uniform(arg_keys[14], (FFW,), jnp.float32) ** steps_of(arg_keys[14], (FFW,), ((0, 4),), -0.2, 0.2)), 0.0001118034, 0.00041926274)
    up_scale = jnp.clip(jnp.exp(math.log(0.00041926274) - 1.32175583 * jax.random.uniform(arg_keys[15], (FFW,), jnp.float32) ** steps_of(arg_keys[15], (FFW,), ((0, 4),), -0.2, 0.2)), 0.0001118034, 0.00041926274)
    w_down = set_ends(jax.random.randint(arg_keys[16], (FFW // 4, D), -2147483648, 2147483647), jax.random.fold_in(arg_keys[16], 1), -2147483648, 2147483646).astype(jnp.int32)
    down_scale = jnp.clip(jnp.exp(jax.random.uniform(arg_keys[17], (D,), jnp.float32, math.log(0.00013258251), math.log(0.00053033006))), 0.00013258251, 0.00053033006)
    return dict(hidden_in=hidden_in, attn_gain=attn_gain, w_qkv=w_qkv, qkv_scale=qkv_scale, q_gain=q_gain, k_gain=k_gain, key_cache=key_cache, value_cache=value_cache, lengths=lengths, w_out=w_out, out_scale=out_scale, mlp_gain=mlp_gain, w_gate=w_gate, w_up=w_up, gate_scale=gate_scale, up_scale=up_scale, w_down=w_down, down_scale=down_scale)


norm_epsilon = 1e-06
rope_base = 1000000.0

def unpack_bytes(packed, byte_index):
    return jnp.right_shift(jnp.left_shift(packed, 24 - 8 * byte_index), 24)

def byte_product(activations, packed):
    products = [jnp.dot(activations[:, byte_index::4], unpack_bytes(packed, byte_index).astype(jnp.bfloat16), preferred_element_type=jnp.float32) for byte_index in range(4)]
    return products[0] + products[1] + products[2] + products[3]

def normalize_rows(values, gain_row):
    return values * lax.rsqrt(lax.optimization_barrier(jnp.mean(values * values, axis=-1, keepdims=True)) + norm_epsilon) * gain_row

def rotary_embed(values, positions):
    half_dim = values.shape[-1] // 2
    freq_index = jnp.arange(half_dim, dtype=jnp.float32)
    inverse = jnp.exp(freq_index * (-math.log(rope_base) / half_dim))
    angles = positions.astype(jnp.float32)[:, None] * inverse[None, :]
    cosine = jnp.cos(angles)[:, None, :]
    sine_part = jnp.sin(angles)[:, None, :]
    lower_half = values[..., :half_dim]
    upper_half = values[..., half_dim:]
    return jnp.concatenate([lower_half * cosine - upper_half * sine_part, upper_half * cosine + lower_half * sine_part], axis=-1)

def attention_rows(query_key_value, q_gain, k_gain, stored_keys, stored_values, seq_lengths):
    count_of_rows = query_key_value.shape[0]
    query_matrix = query_key_value[:, :QUERY_COLUMNS].astype(jnp.float32).reshape(count_of_rows, QUERY_HEADS, HEAD_SIZE)
    incoming_keys = query_key_value[:, QUERY_COLUMNS:QUERY_COLUMNS + KEY_COLUMNS].astype(jnp.float32).reshape(count_of_rows, KEY_VALUE_HEADS, HEAD_SIZE)
    incoming_values = query_key_value[:, QUERY_COLUMNS + KEY_COLUMNS:].reshape(count_of_rows, KEY_VALUE_HEADS, HEAD_SIZE)
    query_matrix = rotary_embed(normalize_rows(query_matrix, q_gain), seq_lengths).astype(jnp.bfloat16)
    incoming_keys = rotary_embed(normalize_rows(incoming_keys, k_gain), seq_lengths).astype(jnp.bfloat16)
    query_groups = query_matrix.astype(jnp.float32).reshape(count_of_rows, KEY_VALUE_HEADS, QUERY_HEADS // KEY_VALUE_HEADS, HEAD_SIZE)
    key_slices = stored_keys.astype(jnp.float32).reshape(count_of_rows, CACHE_POSITIONS, KEY_VALUE_HEADS, HEAD_SIZE)
    value_slices = stored_values.astype(jnp.float32).reshape(count_of_rows, CACHE_POSITIONS, KEY_VALUE_HEADS, HEAD_SIZE)
    logit_scale = 1.0 / math.sqrt(HEAD_SIZE)
    scores = jnp.einsum('bkgd,bpkd->bkgp', query_groups, key_slices) * logit_scale
    live_mask = jnp.arange(CACHE_POSITIONS, dtype=jnp.int32)[None, :] < seq_lengths[:, None]
    scores = jnp.where(live_mask[:, None, None, :], scores, -jnp.inf)
    self_score = jnp.einsum('nufi,nui->nuf', query_groups, incoming_keys.astype(jnp.float32)) * logit_scale
    row_max = jnp.maximum(lax.optimization_barrier(jnp.max(scores, axis=-1)), self_score)
    soft_weights = jnp.exp(scores - row_max[..., None])
    own_weight = jnp.exp(self_score - row_max)
    denominator = lax.optimization_barrier(jnp.sum(soft_weights, axis=-1)) + own_weight
    soft_low = lax.optimization_barrier(soft_weights.astype(jnp.bfloat16)).astype(jnp.float32)
    own_low = lax.optimization_barrier(own_weight.astype(jnp.bfloat16)).astype(jnp.float32)
    numerator = jnp.einsum('bkgp,bpkd->bkgd', soft_low, value_slices) + own_low[..., None] * incoming_values.astype(jnp.float32)[:, :, None, :]
    return (numerator / denominator[..., None]).reshape(count_of_rows, QUERY_COLUMNS).astype(jnp.bfloat16)

def reference(hidden_in, attn_gain, w_qkv, qkv_scale, q_gain, k_gain, key_cache, value_cache, lengths, w_out, out_scale, mlp_gain, w_gate, w_up, gate_scale, up_scale, w_down, down_scale):
    total_rows = hidden_in.shape[0]
    residual = hidden_in.astype(jnp.float32)
    normed = normalize_rows(residual, attn_gain).astype(jnp.bfloat16)
    query_key_value = (byte_product(normed, w_qkv) * qkv_scale).astype(jnp.bfloat16)
    flat_lengths = lengths.reshape(total_rows)
    heads_out = attention_rows(query_key_value, q_gain, k_gain, key_cache.reshape(total_rows, CACHE_POSITIONS, KEY_COLUMNS), value_cache.reshape(total_rows, CACHE_POSITIONS, KEY_COLUMNS), flat_lengths)
    middle = (residual + byte_product(heads_out, w_out) * out_scale).astype(jnp.bfloat16)
    normed_mlp = normalize_rows(middle.astype(jnp.float32), mlp_gain).astype(jnp.bfloat16)
    gate_value = byte_product(normed_mlp, w_gate) * gate_scale
    up_value = byte_product(normed_mlp, w_up) * up_scale
    activated = (jax.nn.silu(gate_value) * up_value).astype(jnp.bfloat16)
    down_value = byte_product(activated, w_down) * down_scale
    return (middle.astype(jnp.float32) + down_value).astype(jnp.bfloat16)
```

```python
import functools
import math

import jax
import jax.numpy as jnp
from jax import lax
from jax.experimental import pallas as pl
from jax.experimental.pallas import tpu as pltpu
from jax.sharding import PartitionSpec as P

D = 5120
QUERY_HEADS = 32
KEY_VALUE_HEADS = 4
HEAD_SIZE = 128
QUERY_COLUMNS = 4096
KEY_COLUMNS = 512


norm_epsilon = 1e-06
rope_base = 1000000.0


def unpack_bytes(packed, byte_index):
    return jnp.right_shift(jnp.left_shift(packed, 24 - 8 * byte_index), 24)


def byte_order(block):
    source = lax.broadcasted_iota(jnp.int32, (block, block), 0)
    target = lax.broadcasted_iota(jnp.int32, (block, block), 1)
    return (target == (source % 4) * (block // 4) + source // 4).astype(jnp.bfloat16)


def split_kernel(block, x_ref, order_ref, out_ref):
    lanes = block // 4
    for c in range(x_ref.shape[1] // block):
        moved = jnp.dot(
            x_ref[:, c * block : (c + 1) * block],
            order_ref[...],
            preferred_element_type=jnp.float32,
        ).astype(jnp.bfloat16)
        for j in range(4):
            out_ref[j, :, c * lanes : (c + 1) * lanes] = moved[:, j * lanes : (j + 1) * lanes]


def split_bytes(activations):
    rows, width = activations.shape
    if width % 512:
        return [activations[:, byte_index::4] for byte_index in range(4)]
    split = pl.pallas_call(
        functools.partial(split_kernel, 512),
        out_shape=jax.ShapeDtypeStruct((4, rows, width // 4), jnp.bfloat16),
        cost_estimate=pl.CostEstimate(
            flops=2 * rows * width * 512, bytes_accessed=4 * rows * width, transcendentals=0
        ),
        name="split_bytes",
    )(activations, byte_order(512))
    return [split[byte_index] for byte_index in range(4)]


def byte_product(activations, packed):
    pieces = split_bytes(activations)
    products = [
        jnp.dot(
            pieces[byte_index],
            unpack_bytes(packed, byte_index).astype(jnp.bfloat16),
            preferred_element_type=jnp.float32,
        )
        for byte_index in range(4)
    ]
    return products[0] + products[1] + products[2] + products[3]


def block_of(width):
    return math.gcd(640, width)


def order_kernel(block, x_ref, order_ref, out_ref):
    for c in range(x_ref.shape[1] // block):
        out_ref[:, c * block : (c + 1) * block] = jnp.dot(
            x_ref[:, c * block : (c + 1) * block],
            order_ref[...],
            preferred_element_type=jnp.float32,
        ).astype(jnp.bfloat16)


def order_bytes(activations):
    rows, width = activations.shape
    block = block_of(width)
    if block == width:
        return jnp.dot(activations, byte_order(block), preferred_element_type=jnp.float32).astype(
            jnp.bfloat16
        )
    return pl.pallas_call(
        functools.partial(order_kernel, block),
        out_shape=jax.ShapeDtypeStruct((rows, width), jnp.bfloat16),
        cost_estimate=pl.CostEstimate(
            flops=2 * rows * width * block, bytes_accessed=4 * rows * width, transcendentals=0
        ),
        name="order_bytes",
    )(activations, byte_order(block))


def unpack_ordered(packed):
    rows, columns = packed.shape
    block = block_of(4 * rows) // 4
    blocks = packed.reshape(rows // block, block, columns)
    parts = [unpack_bytes(blocks, j).astype(jnp.bfloat16) for j in range(4)]
    return jnp.stack(parts, axis=1).reshape(4 * rows, columns)


def normalize_rows(values, gain_row):
    return (
        values
        * lax.rsqrt(jnp.mean(values * values, axis=-1, keepdims=True) + norm_epsilon)
        * gain_row
    )


def rotary_embed(values, positions):
    half_dim = values.shape[-1] // 2
    freq_index = jnp.arange(half_dim, dtype=jnp.float32)
    inverse = jnp.exp(freq_index * (-math.log(rope_base) / half_dim))
    angles = positions.astype(jnp.float32)[:, None] * inverse[None, :]
    cosine = jnp.cos(angles)[:, None, :]
    sine_part = jnp.sin(angles)[:, None, :]
    lower_half = values[..., :half_dim]
    upper_half = values[..., half_dim:]
    return jnp.concatenate(
        [
            lower_half * cosine - upper_half * sine_part,
            upper_half * cosine + lower_half * sine_part,
        ],
        axis=-1,
    )


def local_attention(query_key_value_rows, q_gain, k_gain, stored_keys, stored_values, seq_lengths):
    count_of_rows = query_key_value_rows.shape[0]
    cache_length = stored_keys.shape[1]
    query_matrix = (
        query_key_value_rows[:, :QUERY_COLUMNS]
        .astype(jnp.float32)
        .reshape(count_of_rows, QUERY_HEADS, HEAD_SIZE)
    )
    incoming_keys = (
        query_key_value_rows[:, QUERY_COLUMNS : QUERY_COLUMNS + KEY_COLUMNS]
        .astype(jnp.float32)
        .reshape(count_of_rows, KEY_VALUE_HEADS, HEAD_SIZE)
    )
    incoming_values = query_key_value_rows[:, QUERY_COLUMNS + KEY_COLUMNS :].reshape(
        count_of_rows, KEY_VALUE_HEADS, HEAD_SIZE
    )
    query_matrix = rotary_embed(normalize_rows(query_matrix, q_gain), seq_lengths).astype(
        jnp.bfloat16
    )
    incoming_keys = rotary_embed(normalize_rows(incoming_keys, k_gain), seq_lengths).astype(
        jnp.bfloat16
    )
    query_groups = query_matrix.reshape(
        count_of_rows, KEY_VALUE_HEADS, QUERY_HEADS // KEY_VALUE_HEADS, HEAD_SIZE
    )
    key_slices = stored_keys.reshape(count_of_rows, cache_length, KEY_VALUE_HEADS, HEAD_SIZE)
    value_slices = stored_values.reshape(count_of_rows, cache_length, KEY_VALUE_HEADS, HEAD_SIZE)
    logit_scale = 1.0 / math.sqrt(HEAD_SIZE)
    scores = (
        jnp.einsum("bkgd,bpkd->bkgp", query_groups, key_slices, preferred_element_type=jnp.float32)
        * logit_scale
    )
    live_mask = jnp.arange(cache_length, dtype=jnp.int32)[None, :] < seq_lengths[:, None]
    scores = jnp.where(live_mask[:, None, None, :], scores, -jnp.inf)
    self_score = (
        jnp.einsum("nufi,nui->nuf", query_groups, incoming_keys, preferred_element_type=jnp.float32)
        * logit_scale
    )
    row_max = jnp.maximum(jnp.max(scores, axis=-1), self_score)
    soft_weights = jnp.exp(scores - row_max[..., None])
    own_weight = jnp.exp(self_score - row_max)
    denominator = jnp.sum(soft_weights, axis=-1) + own_weight
    own_low = lax.optimization_barrier(own_weight.astype(jnp.bfloat16)).astype(jnp.float32)
    numerator = jnp.einsum(
        "bkgp,bpkd->bkgd",
        soft_weights.astype(jnp.bfloat16),
        value_slices,
        preferred_element_type=jnp.float32,
    )
    numerator = numerator + own_low[..., None] * incoming_values.astype(jnp.float32)[:, :, None, :]
    return (
        (numerator / denominator[..., None])
        .reshape(count_of_rows, QUERY_COLUMNS)
        .astype(jnp.bfloat16)
    )


def summed_share(terms, tp_count):
    rows, columns = terms.shape
    pieces = lax.all_to_all(terms, "tp", split_axis=1, concat_axis=0, tiled=True)
    return jnp.sum(
        pieces.reshape(tp_count, rows, columns // tp_count).astype(jnp.float32), axis=0
    )


def local(
    hidden_in,
    attn_gain,
    w_qkv,
    qkv_scale,
    q_gain,
    k_gain,
    key_cache,
    value_cache,
    lengths,
    w_out,
    out_scale,
    mlp_gain,
    w_gate,
    w_up,
    gate_scale,
    up_scale,
    w_down,
    down_scale,
):
    tp_count = lax.axis_size("tp")
    tp_index = lax.axis_index("tp")
    share_cols = D // tp_count
    residual = hidden_in.astype(jnp.float32)
    normed = normalize_rows(residual, attn_gain).astype(jnp.bfloat16)
    qkv_part = (byte_product(normed, w_qkv) * qkv_scale).astype(jnp.bfloat16)
    query_key_value_rows = lax.all_to_all(qkv_part, "tp", split_axis=0, concat_axis=1, tiled=True)
    heads_out = local_attention(
        query_key_value_rows, q_gain, k_gain, key_cache[0], value_cache[0], lengths[0]
    )
    head_rows = lax.all_to_all(heads_out, "tp", split_axis=1, concat_axis=0, tiled=True)
    partial_value = (byte_product(head_rows, w_out) * out_scale).astype(jnp.bfloat16)
    residual_share = lax.dynamic_slice_in_dim(hidden_in, tp_index * share_cols, share_cols, 1)
    mid_share = (
        residual_share.astype(jnp.float32) + summed_share(partial_value, tp_count)
    ).astype(jnp.bfloat16)
    mid_full = lax.all_gather(mid_share, "tp", axis=1, tiled=True)
    normed_mlp = normalize_rows(mid_full.astype(jnp.float32), mlp_gain).astype(jnp.bfloat16)
    mlp_columns = order_bytes(
        lax.all_to_all(normed_mlp, ("grp", "src"), split_axis=1, concat_axis=0, tiled=True)
    )
    gate_terms = jnp.dot(mlp_columns, unpack_ordered(w_gate), preferred_element_type=jnp.float32)
    up_terms = jnp.dot(mlp_columns, unpack_ordered(w_up), preferred_element_type=jnp.float32)
    both_terms = jnp.concatenate(
        [gate_terms.astype(jnp.bfloat16), up_terms.astype(jnp.bfloat16)], axis=1
    )
    both = lax.psum_scatter(both_terms, ("grp", "src"), scatter_dimension=0, tiled=True).astype(
        jnp.float32
    )
    hidden = gate_scale.shape[0]
    gate_value = both[:, :hidden] * gate_scale
    up_value = both[:, hidden:] * up_scale
    activated = order_bytes((jax.nn.silu(gate_value) * up_value).astype(jnp.bfloat16))
    all_activated = lax.all_gather(activated, ("grp", "src"), axis=0, tiled=True)
    down_columns = jnp.dot(
        all_activated, unpack_ordered(w_down), preferred_element_type=jnp.float32
    ).astype(jnp.bfloat16)
    down_rows = lax.all_to_all(
        down_columns, ("grp", "src"), split_axis=0, concat_axis=1, tiled=True
    )
    down_share = lax.dynamic_slice_in_dim(down_scale, tp_index * share_cols, share_cols, 0)
    mlp_share = summed_share(down_rows, tp_count) * down_share
    return (mid_share.astype(jnp.float32) + mlp_share).astype(jnp.bfloat16)


def solution(mesh):
    return jax.shard_map(
        local,
        mesh=mesh,
        in_specs=(
            P(("grp", "src"), None),
            P(),
            P(None, "tp"),
            P("tp"),
            P(),
            P(),
            P(("grp", "src"), "tp", None, None),
            P(("grp", "src"), "tp", None, None),
            P(("grp", "src"), "tp"),
            P("tp", None),
            P(),
            P(),
            P(("grp", "src"), "tp"),
            P(("grp", "src"), "tp"),
            P("tp"),
            P("tp"),
            P("tp", ("grp", "src")),
            P(),
        ),
        out_specs=P(("grp", "src"), "tp"),
        check_vma=False,
    )
```

```python
import functools
import math

import jax
import jax.numpy as jnp
from jax import lax
from jax.experimental import pallas as pl
from jax.experimental.pallas import tpu as pltpu
from jax.sharding import PartitionSpec as P

D = 5120
QUERY_HEADS = 32
KEY_VALUE_HEADS = 4
HEAD_SIZE = 128
QUERY_COLUMNS = 4096
KEY_COLUMNS = 512


norm_epsilon = 1e-06
rope_base = 1000000.0


def unpack_bytes(packed, byte_index):
    return jnp.right_shift(jnp.left_shift(packed, 24 - 8 * byte_index), 24)


def byte_order(block):
    source = lax.broadcasted_iota(jnp.int32, (block, block), 0)
    target = lax.broadcasted_iota(jnp.int32, (block, block), 1)
    return (target == (source % 4) * (block // 4) + source // 4).astype(jnp.bfloat16)


def split_kernel(block, x_ref, order_ref, out_ref):
    lanes = block // 4
    for c in range(x_ref.shape[1] // block):
        moved = jnp.dot(
            x_ref[:, c * block : (c + 1) * block],
            order_ref[...],
            preferred_element_type=jnp.float32,
        ).astype(jnp.bfloat16)
        for j in range(4):
            out_ref[j, :, c * lanes : (c + 1) * lanes] = moved[:, j * lanes : (j + 1) * lanes]


def split_bytes(activations):
    rows, width = activations.shape
    if width % 512:
        return [activations[:, byte_index::4] for byte_index in range(4)]
    split = pl.pallas_call(
        functools.partial(split_kernel, 512),
        out_shape=jax.ShapeDtypeStruct((4, rows, width // 4), jnp.bfloat16),
        cost_estimate=pl.CostEstimate(
            flops=2 * rows * width * 512, bytes_accessed=4 * rows * width, transcendentals=0
        ),
        name="split_bytes",
    )(activations, byte_order(512))
    return [split[byte_index] for byte_index in range(4)]


def byte_product(activations, packed):
    pieces = split_bytes(activations)
    products = [
        jnp.dot(
            pieces[byte_index],
            unpack_bytes(packed, byte_index).astype(jnp.bfloat16),
            preferred_element_type=jnp.float32,
        )
        for byte_index in range(4)
    ]
    return products[0] + products[1] + products[2] + products[3]


def block_of(width):
    return math.gcd(640, width)


def order_kernel(block, x_ref, order_ref, out_ref):
    for c in range(x_ref.shape[1] // block):
        out_ref[:, c * block : (c + 1) * block] = jnp.dot(
            x_ref[:, c * block : (c + 1) * block],
            order_ref[...],
            preferred_element_type=jnp.float32,
        ).astype(jnp.bfloat16)


def order_bytes(activations):
    rows, width = activations.shape
    block = block_of(width)
    if block == width:
        return jnp.dot(activations, byte_order(block), preferred_element_type=jnp.float32).astype(
            jnp.bfloat16
        )
    return pl.pallas_call(
        functools.partial(order_kernel, block),
        out_shape=jax.ShapeDtypeStruct((rows, width), jnp.bfloat16),
        cost_estimate=pl.CostEstimate(
            flops=2 * rows * width * block, bytes_accessed=4 * rows * width, transcendentals=0
        ),
        name="order_bytes",
    )(activations, byte_order(block))


def unpack_ordered(packed):
    rows, columns = packed.shape
    block = block_of(4 * rows) // 4
    blocks = packed.reshape(rows // block, block, columns)
    parts = [unpack_bytes(blocks, j).astype(jnp.bfloat16) for j in range(4)]
    return jnp.stack(parts, axis=1).reshape(4 * rows, columns)


def normalize_rows(values, gain_row):
    return (
        values
        * lax.rsqrt(jnp.mean(values * values, axis=-1, keepdims=True) + norm_epsilon)
        * gain_row
    )


def rotary_embed(values, positions):
    half_dim = values.shape[-1] // 2
    freq_index = jnp.arange(half_dim, dtype=jnp.float32)
    inverse = jnp.exp(freq_index * (-math.log(rope_base) / half_dim))
    angles = positions.astype(jnp.float32)[:, None] * inverse[None, :]
    cosine = jnp.cos(angles)[:, None, :]
    sine_part = jnp.sin(angles)[:, None, :]
    lower_half = values[..., :half_dim]
    upper_half = values[..., half_dim:]
    return jnp.concatenate(
        [
            lower_half * cosine - upper_half * sine_part,
            upper_half * cosine + lower_half * sine_part,
        ],
        axis=-1,
    )


def local_attention(query_key_value_rows, q_gain, k_gain, stored_keys, stored_values, seq_lengths):
    count_of_rows = query_key_value_rows.shape[0]
    cache_length = stored_keys.shape[1]
    query_matrix = (
        query_key_value_rows[:, :QUERY_COLUMNS]
        .astype(jnp.float32)
        .reshape(count_of_rows, QUERY_HEADS, HEAD_SIZE)
    )
    incoming_keys = (
        query_key_value_rows[:, QUERY_COLUMNS : QUERY_COLUMNS + KEY_COLUMNS]
        .astype(jnp.float32)
        .reshape(count_of_rows, KEY_VALUE_HEADS, HEAD_SIZE)
    )
    incoming_values = query_key_value_rows[:, QUERY_COLUMNS + KEY_COLUMNS :].reshape(
        count_of_rows, KEY_VALUE_HEADS, HEAD_SIZE
    )
    query_matrix = rotary_embed(normalize_rows(query_matrix, q_gain), seq_lengths).astype(
        jnp.bfloat16
    )
    incoming_keys = rotary_embed(normalize_rows(incoming_keys, k_gain), seq_lengths).astype(
        jnp.bfloat16
    )
    query_groups = query_matrix.reshape(
        count_of_rows, KEY_VALUE_HEADS, QUERY_HEADS // KEY_VALUE_HEADS, HEAD_SIZE
    )
    key_slices = stored_keys.reshape(count_of_rows, cache_length, KEY_VALUE_HEADS, HEAD_SIZE)
    value_slices = stored_values.reshape(count_of_rows, cache_length, KEY_VALUE_HEADS, HEAD_SIZE)
    logit_scale = 1.0 / math.sqrt(HEAD_SIZE)
    scores = (
        jnp.einsum("bkgd,bpkd->bkgp", query_groups, key_slices, preferred_element_type=jnp.float32)
        * logit_scale
    )
    live_mask = jnp.arange(cache_length, dtype=jnp.int32)[None, :] < seq_lengths[:, None]
    scores = jnp.where(live_mask[:, None, None, :], scores, -jnp.inf)
    self_score = (
        jnp.einsum("nufi,nui->nuf", query_groups, incoming_keys, preferred_element_type=jnp.float32)
        * logit_scale
    )
    row_max = jnp.maximum(jnp.max(scores, axis=-1), self_score)
    soft_weights = jnp.exp(scores - row_max[..., None])
    own_weight = jnp.exp(self_score - row_max)
    denominator = jnp.sum(soft_weights, axis=-1) + own_weight
    own_low = lax.optimization_barrier(own_weight.astype(jnp.bfloat16)).astype(jnp.float32)
    numerator = jnp.einsum(
        "bkgp,bpkd->bkgd",
        soft_weights.astype(jnp.bfloat16),
        value_slices,
        preferred_element_type=jnp.float32,
    )
    numerator = numerator + own_low[..., None] * incoming_values.astype(jnp.float32)[:, :, None, :]
    return (
        (numerator / denominator[..., None])
        .reshape(count_of_rows, QUERY_COLUMNS)
        .astype(jnp.bfloat16)
    )


def summed_share(terms, tp_count):
    rows, columns = terms.shape
    pieces = lax.all_to_all(terms, "tp", split_axis=1, concat_axis=0, tiled=True)
    return jnp.sum(
        pieces.reshape(tp_count, rows, columns // tp_count).astype(jnp.float32), axis=0
    )


def gathered_rows(rows, axis):
    count = lax.axis_size(axis)
    copies = jnp.broadcast_to(rows[None], (count, *rows.shape))
    pieces = lax.all_to_all(copies, axis, split_axis=0, concat_axis=0)
    return pieces.reshape(count * rows.shape[0], rows.shape[1])


def summed_rows(terms, axis):
    count = lax.axis_size(axis)
    rows, columns = terms.shape
    pieces = lax.all_to_all(
        terms.reshape(count, rows // count, columns), axis, split_axis=0, concat_axis=0
    )
    return jnp.sum(pieces.astype(jnp.float32), axis=0)


def local(
    hidden_in,
    attn_gain,
    w_qkv,
    qkv_scale,
    q_gain,
    k_gain,
    key_cache,
    value_cache,
    lengths,
    w_out,
    out_scale,
    mlp_gain,
    w_gate,
    w_up,
    gate_scale,
    up_scale,
    w_down,
    down_scale,
):
    tp_count = lax.axis_size("tp")
    tp_index = lax.axis_index("tp")
    share_cols = D // tp_count
    residual = hidden_in.astype(jnp.float32)
    normed = normalize_rows(residual, attn_gain).astype(jnp.bfloat16)
    qkv_part = (byte_product(normed, w_qkv) * qkv_scale).astype(jnp.bfloat16)
    query_key_value_rows = lax.all_to_all(qkv_part, "tp", split_axis=0, concat_axis=1, tiled=True)
    heads_out = local_attention(
        query_key_value_rows, q_gain, k_gain, key_cache[0], value_cache[0], lengths[0]
    )
    head_rows = lax.all_to_all(heads_out, "tp", split_axis=1, concat_axis=0, tiled=True)
    partial_value = (byte_product(head_rows, w_out) * out_scale).astype(jnp.bfloat16)
    residual_share = lax.dynamic_slice_in_dim(hidden_in, tp_index * share_cols, share_cols, 1)
    mid_share = (
        residual_share.astype(jnp.float32) + summed_share(partial_value, tp_count)
    ).astype(jnp.bfloat16)
    mid_full = lax.all_gather(mid_share, "tp", axis=1, tiled=True)
    normed_mlp = normalize_rows(mid_full.astype(jnp.float32), mlp_gain).astype(jnp.bfloat16)
    mlp_columns = order_bytes(
        lax.all_to_all(normed_mlp, ("grp", "src"), split_axis=1, concat_axis=0, tiled=True)
    )
    gate_terms = jnp.dot(mlp_columns, unpack_ordered(w_gate), preferred_element_type=jnp.float32)
    up_terms = jnp.dot(mlp_columns, unpack_ordered(w_up), preferred_element_type=jnp.float32)
    both_terms = jnp.concatenate(
        [gate_terms.astype(jnp.bfloat16), up_terms.astype(jnp.bfloat16)], axis=1
    )
    both = summed_rows(summed_rows(both_terms, "grp").astype(jnp.bfloat16), "src")
    hidden = gate_scale.shape[0]
    gate_value = both[:, :hidden] * gate_scale
    up_value = both[:, hidden:] * up_scale
    activated = order_bytes((jax.nn.silu(gate_value) * up_value).astype(jnp.bfloat16))
    all_activated = gathered_rows(gathered_rows(activated, "src"), "grp")
    down_columns = jnp.dot(
        all_activated, unpack_ordered(w_down), preferred_element_type=jnp.float32
    ).astype(jnp.bfloat16)
    down_rows = lax.all_to_all(
        down_columns, ("grp", "src"), split_axis=0, concat_axis=1, tiled=True
    )
    down_share = lax.dynamic_slice_in_dim(down_scale, tp_index * share_cols, share_cols, 0)
    mlp_share = summed_share(down_rows, tp_count) * down_share
    return (mid_share.astype(jnp.float32) + mlp_share).astype(jnp.bfloat16)


def solution(mesh):
    return jax.shard_map(
        local,
        mesh=mesh,
        in_specs=(
            P(("grp", "src"), None),
            P(),
            P(None, "tp"),
            P("tp"),
            P(),
            P(),
            P(("grp", "src"), "tp", None, None),
            P(("grp", "src"), "tp", None, None),
            P(("grp", "src"), "tp"),
            P("tp", None),
            P(),
            P(),
            P(("grp", "src"), "tp"),
            P(("grp", "src"), "tp"),
            P("tp"),
            P("tp"),
            P("tp", ("grp", "src")),
            P(),
        ),
        out_specs=P(("grp", "src"), "tp"),
        check_vma=False,
    )
```
